16 devices in a mesh: dp: 4 (over y, z, core), sp: 4 (over x).
Axes of the slice: x: 4, y: 2, z: 1, core: 2. Of those that a mesh axis runs over, the one named last changes fastest.
The devices are a block of a 4x4x8 slice.
Arguments:
- x: bfloat16 [16384, 3072], P(('dp', 'sp')), parts along dimension 0
- gain: bfloat16 [3072], replicated
- wq: bfloat16 [3072, 3072], P('sp')
- wk: bfloat16 [3072, 1024], P('sp')
- wv: bfloat16 [3072, 1024], P('sp')
- wo: bfloat16 [3072, 3072], P('sp')
Outputs:
- output: bfloat16 [16384, 3072], P(('dp', 'sp')), parts along dimension 0
There are 4 independent parts. The reference program is written for one: setup_inputs(seed, part) draws one part's arguments, and reference() takes and returns one part's arrays. A program takes and returns all parts, laid end to end along the dimension named above; an argument that names none is the same for every part.
All inputs are finite; a program needn't handle non-finite values.
Results may differ from the reference program's by a relative error of at most 0.012.
Values are sent between devices in bfloat16 or wider.
A program may use at most 768 MiB of HBM per device.

```python
import jax
import jax.numpy as jnp
from jax import lax

ROWS = 4096
D = 3072
HEADS = 24
KV_HEADS = 8
HEAD = 128
THETA = 10000


def setup_inputs(seed: int = 0, part: int = 0) -> dict:
    kx, kn, kq, kk, kv, ko = jax.random.split(jax.random.key(seed), 6)

    def weights(key, rows, columns):
        return jax.random.normal(key, (rows, columns), jnp.float32) * rows**-0.5

    drawn = {
        "x": jax.random.normal(jax.random.fold_in(kx, part), (ROWS, D), jnp.float32),
        "gain": 1 + 0.1 * jax.random.normal(kn, (D,), jnp.float32),
        "wq": 2 * weights(kq, D, HEADS * HEAD),
        "wk": 2 * weights(kk, D, KV_HEADS * HEAD),
        "wv": 4 * weights(kv, D, KV_HEADS * HEAD),
        "wo": weights(ko, HEADS * HEAD, D),
    }
    return {k: v.astype(jnp.bfloat16) for k, v in drawn.items()}


def normed(x, gain):
    wide = x.astype(jnp.float32)
    scale = lax.rsqrt(jnp.mean(wide * wide, -1, keepdims=True) + 1e-6)
    return (wide * scale * gain.astype(jnp.float32)).astype(jnp.bfloat16)


def turned(t, place, theta):
    half = t.shape[-1] // 2
    angle = place.astype(jnp.float32)[:, None] * theta ** (-jnp.arange(half, dtype=jnp.float32) / half)
    cos, sin = jnp.cos(angle)[:, None], jnp.sin(angle)[:, None]
    a, b = t[..., :half].astype(jnp.float32), t[..., half:].astype(jnp.float32)
    return jnp.concatenate([a * cos - b * sin, b * cos + a * sin], -1).astype(jnp.bfloat16)


def matmul(a, w):
    return jnp.dot(a, w, preferred_element_type=jnp.float32).astype(jnp.bfloat16)


def einsum(form, a, b):
    return jnp.einsum(form, a.astype(jnp.float32), b.astype(jnp.float32))


def attention(q, k, v):
    scores = einsum("tgsd,ugd->gstu", q, k) * q.shape[-1] ** -0.5
    token = jnp.arange(q.shape[0])
    scores = jnp.where(token[:, None] >= token, scores, -jnp.inf)
    weights = jax.nn.softmax(scores, -1).astype(jnp.bfloat16)
    return einsum("gstu,ugd->tgsd", weights, v).astype(jnp.bfloat16)


def reference(x, gain, wq, wk, wv, wo):
    a, place = normed(x, gain), jnp.arange(ROWS)
    q = turned(matmul(a, wq).reshape(ROWS, HEADS, HEAD), place, THETA).reshape(ROWS, KV_HEADS, -1, HEAD)
    k = turned(matmul(a, wk).reshape(ROWS, KV_HEADS, HEAD), place, THETA)
    v = matmul(a, wv).reshape(ROWS, KV_HEADS, HEAD)
    seen = attention(q, k, v).reshape(ROWS, HEADS * HEAD)
    return (x.astype(jnp.float32) + jnp.dot(seen, wo, preferred_element_type=jnp.float32)).astype(jnp.bfloat16)
```

```python
import functools

import jax
import jax.numpy as jnp
from jax import lax
from jax.experimental import pallas as pl
from jax.experimental.pallas import tpu as pltpu
from jax.sharding import PartitionSpec as P

HEAD = 128
THETA = 10000
LOG2E = 1.4426950408889634
SP = 4
SLOTS = 4
LAG = 2
MESH = pl.DeviceIdType.MESH


def _dot(a, b, ca, cb):
    return lax.dot_general(a, b, (((ca,), (cb,)), ((), ())), preferred_element_type=jnp.float32)


def _al(i, unit):
    return pl.multiple_of(i, unit)


def _kernel(group, x_ref, gain_ref, cos_ref, sin_ref, wq_ref, wk_ref, wv_ref, wo_ref, y_ref, wl, wol,
            a_s, acc_s, o_s, k_s, v_s, q_s, w_s, wo_s, top_s, mix_s,
            sx, rx, sx2, rx2, sy, ry, sc, rc, skv, rkv, local, fetch, wfetch):
    tokens, depth = x_ref.shape
    heads = wk_ref.shape[1] // HEAD
    gw = group * HEAD
    width = gw + 2 * HEAD
    shard = depth // SP
    shard_o = wo_ref.shape[0] // 2
    chunk = depth // SP
    B = tokens // 2
    cols = group * tokens

    s, d = lax.axis_index("sp"), lax.axis_index("dp")
    left, right, opp = lax.rem(s + 3, SP), lax.rem(s + 1, SP), lax.rem(s + 2, SP)
    j = lax.rem(d, 4)
    core = lax.rem(j, 2)
    jc = j + 1 - 2 * core
    jy, jcy = lax.rem(j + 2, 4), lax.rem(jc + 2, 4)
    to_left, to_right = {"sp": left}, {"sp": right}
    to_core = {"dp": d + 1 - 2 * core}
    to_chip = {"dp": d + 2 - 4 * lax.div(j, 2)}
    sources = (left, right, opp)

    def remote(src, dst, send, recv, device):
        return pltpu.make_async_remote_copy(src_ref=src, dst_ref=dst, send_sem=send, recv_sem=recv, device_id=device, device_id_type=MESH)

    def head_of(g):
        return 2 * lax.rem(g, SP) + lax.div(g, SP)

    def piece(st, g, src, jj, part=None):
        if st == 0:
            n = shard // 4
            at, n = (src * shard + jj * n, n) if part is None else (src * shard + jj * n + part * (n // 2), n // 2)
            return wl.at[g, pl.ds(_al(at, 16), n), :]
        n = shard_o // 4
        at, n = (src * shard_o + jj * n, n) if part is None else (src * shard_o + jj * n + part * (n // 2), n // 2)
        return wol.at[lax.div(g, SP), pl.ds(_al(at, 16), n), pl.ds(_al(lax.rem(g, SP) * chunk, 128), chunk)]

    def own(st, g):
        h = head_of(g)
        if st == 0:
            n = shard // 4
            rows, at = pl.ds(_al(j * n, 16), n), pl.ds(_al(s * shard + j * n, 16), n)
            return [(wq_ref.at[rows, pl.ds(_al(h * gw, 128), gw)], wl.at[g, at, pl.ds(0, gw)]),
                    (wk_ref.at[rows, pl.ds(_al(h * HEAD, 128), HEAD)], wl.at[g, at, pl.ds(gw, HEAD)]),
                    (wv_ref.at[rows, pl.ds(_al(h * HEAD, 128), HEAD)], wl.at[g, at, pl.ds(gw + HEAD, HEAD)])]
        n = shard_o // 4
        rows = pl.ds(_al(lax.div(g, SP) * shard_o + j * n, 16), n)
        return [(wo_ref.at[rows, pl.ds(_al(lax.rem(g, SP) * chunk, 128), chunk)], piece(1, g, s, j))]

    def to_chip_copy(st, g, i):
        p = piece(st, g, sources[i], j)
        return remote(p, p, sy.at[st, g, i], ry.at[st, g, i], to_chip)

    def to_core_copy(st, g, i):
        p = piece(st, g, sources[i % 3], j if i < 3 else jy)
        return remote(p, p, sc.at[st, g, i], rc.at[st, g, i], to_core)

    def on(st, g, src, device, way):
        part = piece(st, g, src, j, way)
        return remote(part, part, sx2.at[st, g, way], rx2.at[st, g, way], device)

    def arrived(ref, sem):
        remote(ref, ref, sem, sem, to_core).wait_recv()

    def g0(st, g):
        for way, device in ((0, to_right), (1, to_left)):
            for src, dst in own(st, g):
                remote(src, dst, sx.at[st, g, way], rx.at[st, g, way], device).start()

    def g1(st, g):
        for way, src, device in ((0, left, to_right), (1, right, to_left)):
            arrived(piece(st, g, src, j), rx.at[st, g, way])
            on(st, g, src, device, way).start()
            to_chip_copy(st, g, way).start()
            to_core_copy(st, g, way).start()

    def g2(st, g):
        for way in (0, 1):
            arrived(piece(st, g, opp, j, way), rx2.at[st, g, way])
        to_chip_copy(st, g, 2).start()
        to_core_copy(st, g, 2).start()

    def g3(st, g):
        for i in range(3):
            arrived(piece(st, g, sources[i], jy), ry.at[st, g, i])
            to_core_copy(st, g, 3 + i).start()

    def g4(st, g):
        for i in range(6):
            arrived(piece(st, g, sources[i % 3], jc if i < 3 else jcy), rc.at[st, g, i])

    def both(stage, g):
        @pl.when(g < heads)
        def _():
            stage(0, g)

        @pl.when((g >= LAG) & (g < heads + LAG))
        def _():
            stage(1, g - LAG)

    def sent(st, g):
        for way, src, device in ((0, left, to_right), (1, right, to_left)):
            p = piece(st, g, s, j)
            remote(p, p, sx.at[st, g, way], rx.at[st, g, way], device).wait_send()
            on(st, g, src, device, way).wait_send()
        for i in range(3):
            to_chip_copy(st, g, i).wait_send()
        for i in range(6):
            to_core_copy(st, g, i).wait_send()

    def fetches(g):
        h = head_of(g)
        mine = pl.ds(_al(s * shard, 16), shard)
        out = [pltpu.make_async_copy(wq_ref.at[:, pl.ds(_al(h * gw, 128), gw)], w_s.at[mine, pl.ds(0, gw)], fetch.at[0]),
               pltpu.make_async_copy(wk_ref.at[:, pl.ds(_al(h * HEAD, 128), HEAD)], w_s.at[mine, pl.ds(gw, HEAD)], fetch.at[1]),
               pltpu.make_async_copy(wv_ref.at[:, pl.ds(_al(h * HEAD, 128), HEAD)], w_s.at[mine, pl.ds(gw + HEAD, HEAD)], fetch.at[2])]
        for i, src in enumerate(sources):
            at = pl.ds(_al(src * shard, 16), shard)
            out.append(pltpu.make_async_copy(wl.at[g, at, :], w_s.at[at, :], fetch.at[3 + i]))
        return out

    def wo_fetches(half, c, slot):
        at = pl.ds(_al(c * chunk, 128), chunk)
        mine = pl.ds(_al(s * shard_o, 16), shard_o)
        out = [pltpu.make_async_copy(wo_ref.at[pl.ds(_al(half * shard_o, 16), shard_o), at], wo_s.at[slot, mine, :], wfetch.at[slot, 0])]
        for i, src in enumerate(sources):
            rows = pl.ds(_al(src * shard_o, 16), shard_o)
            out.append(pltpu.make_async_copy(wol.at[half, rows, at], wo_s.at[slot, rows, :], wfetch.at[slot, 1 + i]))
        return out

    def project(g):
        slot, par, m = lax.rem(g, SLOTS), lax.rem(g, 2), B

        def tile(i, _):
            rows = pl.ds(_al(i * m, 128), m)
            r = _dot(a_s[rows, :], w_s[...], 1, 0).astype(jnp.bfloat16)
            cos, sin = cos_ref[rows, :], sin_ref[rows, :]

            def turned(t):
                t = t.astype(jnp.float32)
                return (t * cos + pltpu.roll(t, HEAD // 2, 1) * sin).astype(jnp.bfloat16)

            k_s[slot, s, rows, :] = turned(r[:, gw : gw + HEAD])
            v_s[slot, s, :, rows] = r[:, gw + HEAD :].T
            for n in range(group):
                q_s[par, pl.ds(_al(n * tokens + i * m, 128), m), :] = turned(r[:, n * HEAD : (n + 1) * HEAD])

        lax.fori_loop(0, tokens // m, tile, None)

    def kv(g, src, which, number, device):
        slot = lax.rem(g, SLOTS)
        ref = (k_s if which == 0 else v_s).at[slot, src]
        return remote(ref, ref, skv.at[g, number], rkv.at[g, src, which], device)

    own_kv = (
        (lambda: s < 2, 1, 2, to_left),
        (lambda: s == 0, 0, 3, to_left),
        (lambda: s < 3, 0, 0, to_right),
        (lambda: s < 3, 1, 1, to_right),
    )
    passed_on = ((0, 1, 1, to_left), (1, 0, 0, to_right), (2, 1, 0, to_right), (3, 0, 1, to_left))

    def kv_send(g):
        for who, which, number, device in own_kv:
            @pl.when(who())
            def _():
                kv(g, s, which, number, device).start()

    def kv_on(g):
        for place, src, which, device in passed_on:
            @pl.when(s == place)
            def _():
                copy = kv(g, src, which, 4, device)
                copy.wait_recv()
                copy.start()

    def kv_sent(g):
        for who, which, number, device in own_kv:
            @pl.when(who())
            def _():
                kv(g, s, which, number, device).wait_send()
        for place, src, which, device in passed_on:
            @pl.when(s == place)
            def _():
                kv(g, src, which, 4, device).wait_send()

    e = HEAD**-0.5 * LOG2E

    def block(g, src, kb, strips, first=False, masked=()):
        slot, par = lax.rem(g, SLOTS), lax.rem(g, 2)
        at_k = pl.ds(kb * B if isinstance(kb, int) else _al(kb * B, 128), B)
        k = k_s[slot, src, at_k, :]
        values = jnp.concatenate([v_s[slot, src, :, at_k], jnp.ones((8, B), jnp.bfloat16)], axis=0)
        scores = [_dot(k, q_s[par, at : at + B, :], 1, 1) for at in strips]
        weights, keeps = [], []
        for at, sc_ in zip(strips, scores):
            if at in masked:
                seen = lax.broadcasted_iota(jnp.int32, (B, B), 1) >= lax.broadcasted_iota(jnp.int32, (B, B), 0)
                sc_ = jnp.where(seen, sc_, -1e30)
            top = sc_.max(axis=0, keepdims=True)
            if not first:
                old = top_s[:, at : at + B]
                top = jnp.maximum(old, top)
                keeps.append(jnp.exp2((old - top) * e))
            top_s[:, at : at + B] = top
            weights.append(jnp.exp2((sc_ - top) * e).astype(jnp.bfloat16))
        for n, (at, p) in enumerate(zip(strips, weights)):
            new = _dot(values, p, 1, 0)
            mix_s[:, at : at + B] = new if first else mix_s[:, at : at + B] * keeps[n] + new

    strips = [n * tokens + half * B for n in range(group) for half in (0, 1)]

    def finish(g):
        half, i = lax.div(g, SP), lax.rem(g, SP)
        for n in range(group):
            at = slice(n * tokens, (n + 1) * tokens)
            out = mix_s[:HEAD, at] * (1 / mix_s[HEAD : HEAD + 1, at])
            o_s[half, :, pl.ds(_al(i * gw + n * HEAD, 128), HEAD)] = out.T.astype(jnp.bfloat16)

    barrier = pltpu.get_barrier_semaphore()
    for device in (to_left, to_right, to_core, to_chip):
        pl.semaphore_signal(barrier, inc=1, device_id=device, device_id_type=MESH)
    load = pltpu.make_async_copy(x_ref, a_s, local.at[0])
    load.start()
    pl.semaphore_wait(barrier, 4)
    g0(0, 0)
    g0(0, 1)
    g0(0, 2)
    g0(1, 0)
    load.wait()

    def norm(i, _):
        rows = pl.ds(_al(i * 64, 16), 64)
        wide = a_s[rows, :].astype(jnp.float32)
        acc_s[rows, :] = wide
        scale = lax.rsqrt(jnp.mean(wide * wide, -1, keepdims=True) + 1e-6)
        a_s[rows, :] = (wide * scale * gain_ref[...].astype(jnp.float32)).astype(jnp.bfloat16)

    lax.fori_loop(0, tokens // 64, norm, None)
    g1(0, 0)
    g2(0, 0)
    g1(0, 1)
    g2(0, 1)
    g3(0, 0)
    g4(0, 0)
    for f in fetches(0):
        f.start()
    for f in fetches(0):
        f.wait()
    project(0)
    kv_send(0)
    g3(0, 1)

    def step(t, _):
        @pl.when(t + 1 < heads)
        def _():
            g4(0, t + 1)
            for f in fetches(t + 1):
                f.start()

        @pl.when(t + 1 >= LAG)
        def _():
            g4(1, t + 1 - LAG)

        @pl.when(t >= SP)
        def _():
            for f in wo_fetches(0, t - SP, 0):
                f.start()

        both(g0, t + 3)
        block(t, s, 0, strips, first=True, masked=strips[0::2])
        block(t, s, 1, strips[1::2], masked=strips[1::2])
        kv_on(t)

        @pl.when(t + 1 < heads)
        def _():
            for f in fetches(t + 1):
                f.wait()
            project(t + 1)
            kv_send(t + 1)

        def other(i, _):
            src = jnp.where(i == 1, s - 1, i - 2)

            @pl.when(s >= i)
            def _():
                @pl.when((i > 1) | (s == 3))
                def _():
                    kv(t, src, 0, 5, to_left).wait_recv()

                @pl.when((i != 2) | (s != 3))
                def _():
                    kv(t, src, 1, 5, to_left).wait_recv()

                lax.fori_loop(0, 2, lambda kb, _: block(t, src, kb, strips), None)

            for n, stage in ((1, g1), (2, g2), (3, g3)):
                @pl.when(i == n)
                def _():
                    both(stage, t + 2)

        lax.fori_loop(1, SP, other, None)
        finish(t)
        kv_sent(t)

        @pl.when(t >= SP)
        def _():
            c = t - SP
            for f in wo_fetches(0, c, 0):
                f.wait()

            def tile(i, _):
                rows, at = pl.ds(_al(i * B, 128), B), pl.ds(_al(c * chunk, 128), chunk)
                acc_s[rows, at] += _dot(o_s[0, rows, :], wo_s[0], 1, 0)

            lax.fori_loop(0, tokens // B, tile, None)

    lax.fori_loop(0, heads, step, None)

    for f in wo_fetches(1, 0, 0):
        f.start()
    g4(1, heads - 1)

    def last(c, _):
        slot = lax.rem(c, 2)

        @pl.when(c + 1 < SP)
        def _():
            for f in wo_fetches(1, c + 1, 1 - slot):
                f.start()

        for f in wo_fetches(1, c, slot):
            f.wait()
        at = pl.ds(_al(c * chunk, 128), chunk)

        def tile(i, _):
            rows = pl.ds(_al(i * B, 128), B)
            a_s[rows, at] = (acc_s[rows, at] + _dot(o_s[1, rows, :], wo_s[slot], 1, 0)).astype(jnp.bfloat16)

        lax.fori_loop(0, tokens // B, tile, None)
        pltpu.make_async_copy(a_s.at[:, at], y_ref.at[:, at], local.at[c]).start()

    lax.fori_loop(0, SP, last, None)

    def drain(g, _):
        sent(0, g)
        sent(1, g)

    lax.fori_loop(0, heads, drain, None)
    for c in range(SP):
        at = pl.ds(c * chunk, chunk)
        pltpu.make_async_copy(a_s.at[:, at], y_ref.at[:, at], local.at[c]).wait()


def solution(mesh):
    def step(x, gain, wq, wk, wv, wo):
        tokens, depth = x.shape
        heads, group = wk.shape[1] // HEAD, wq.shape[1] // wk.shape[1]
        half = HEAD // 2
        place = lax.axis_index("sp") * tokens + jnp.arange(tokens)
        angle = place.astype(jnp.float32)[:, None] * THETA ** (-jnp.arange(half, dtype=jnp.float32) / half)
        cos, sin = jnp.cos(angle), jnp.sin(angle)
        cos, sin = jnp.concatenate([cos, cos], -1), jnp.concatenate([-sin, sin], -1)
        width, B = (group + 2) * HEAD, tokens // 2
        low, wide = jnp.bfloat16, jnp.float32
        half_o = wo.shape[0] // 2 * SP
        anywhere, vmem = pl.BlockSpec(memory_space=pl.ANY), pl.BlockSpec(memory_space=pltpu.VMEM)
        dma = pltpu.SemaphoreType.DMA
        flops = 2 * tokens * depth * (wq.shape[1] * 2 + 2 * wk.shape[1]) + 4 * tokens * tokens * wq.shape[1] * SP
        y, _, _ = pl.pallas_call(
            functools.partial(_kernel, group),
            out_shape=[jax.ShapeDtypeStruct(x.shape, low), jax.ShapeDtypeStruct((heads, depth, width), low),
                       jax.ShapeDtypeStruct((2, half_o, depth), low)],
            in_specs=[anywhere, vmem, vmem, vmem, anywhere, anywhere, anywhere, anywhere],
            out_specs=[anywhere, anywhere, anywhere],
            scratch_shapes=[
                pltpu.VMEM((tokens, depth), low),
                pltpu.VMEM((tokens, depth), wide),
                pltpu.VMEM((2, tokens, half_o), low),
                pltpu.VMEM((SLOTS, SP, tokens, HEAD), low),
                pltpu.VMEM((SLOTS, SP, HEAD, tokens), low),
                pltpu.VMEM((2, group * tokens, HEAD), low),
                pltpu.VMEM((depth, width), low),
                pltpu.VMEM((2, half_o, depth // SP), low),
                pltpu.VMEM((1, group * tokens), wide),
                pltpu.VMEM((HEAD + 8, group * tokens), wide),
                dma((2, heads, 2)), dma((2, heads, 2)), dma((2, heads, 2)), dma((2, heads, 2)),
                dma((2, heads, 3)), dma((2, heads, 3)), dma((2, heads, 6)), dma((2, heads, 6)),
                dma((heads, 6)), dma((heads, SP, 2)), dma((SP,)), dma((6,)), dma((2, SP)),
            ],
            compiler_params=pltpu.CompilerParams(collective_id=0, has_side_effects=True, vmem_limit_bytes=67043328),
            cost_estimate=pl.CostEstimate(flops=flops, transcendentals=tokens * tokens * 2 * heads * group, bytes_accessed=200 * 2**20),
        )(x, gain[None, :], cos, sin, wq, wk, wv, wo)
        return y

    tokens, whole = P(("dp", "sp"), None), P("sp", None)
    return jax.shard_map(
        step,
        mesh=mesh,
        in_specs=(tokens, P(None), whole, whole, whole, whole),
        out_specs=tokens,
        check_vma=False,
    )
```

```python
import functools

import jax
import jax.numpy as jnp
from jax import lax
from jax.experimental import pallas as pl
from jax.experimental.pallas import tpu as pltpu
from jax.sharding import PartitionSpec as P

HEAD = 128
THETA = 10000
LOG2E = 1.4426950408889634
SP = 4
SLOTS = 6
LAG = 2
MESH = pl.DeviceIdType.MESH


def _dot(a, b, ca, cb):
    return lax.dot_general(a, b, (((ca,), (cb,)), ((), ())), preferred_element_type=jnp.float32)


def _al(i, unit):
    return pl.multiple_of(i, unit)


def _kernel(group, x_ref, gain_ref, cos_ref, sin_ref, wq_ref, wk_ref, wv_ref, wo_ref, y_ref, wl, wol,
            a_s, acc_s, o_s, k_s, v_s, q_s, w_s, wo_s, top_s, mix_s,
            sx, rx, sx2, rx2, sy, ry, sc, rc, skv, rkv, local, fetch, wfetch):
    tokens, depth = x_ref.shape
    heads = wk_ref.shape[1] // HEAD
    gw = group * HEAD
    width = gw + 2 * HEAD
    shard = depth // SP
    shard_o = wo_ref.shape[0] // 2
    chunk = depth // SP
    B = tokens // 2
    cols = group * tokens

    s, d = lax.axis_index("sp"), lax.axis_index("dp")
    left, right, opp = lax.rem(s + 3, SP), lax.rem(s + 1, SP), lax.rem(s + 2, SP)
    j = lax.rem(d, 4)
    core = lax.rem(j, 2)
    jc = j + 1 - 2 * core
    jy, jcy = lax.rem(j + 2, 4), lax.rem(jc + 2, 4)
    to_left, to_right = {"sp": left}, {"sp": right}
    to_core = {"dp": d + 1 - 2 * core}
    to_chip = {"dp": d + 2 - 4 * lax.div(j, 2)}
    sources = (left, right, opp)

    def remote(src, dst, send, recv, device):
        return pltpu.make_async_remote_copy(src_ref=src, dst_ref=dst, send_sem=send, recv_sem=recv, device_id=device, device_id_type=MESH)

    def head_of(g):
        return 2 * lax.rem(g, SP) + lax.div(g, SP)

    def piece(st, g, src, jj, part=None):
        if st == 0:
            n = shard // 4
            at, n = (src * shard + jj * n, n) if part is None else (src * shard + jj * n + part * (n // 2), n // 2)
            return wl.at[g, pl.ds(_al(at, 16), n), :]
        n = shard_o // 4
        at, n = (src * shard_o + jj * n, n) if part is None else (src * shard_o + jj * n + part * (n // 2), n // 2)
        return wol.at[lax.div(g, SP), pl.ds(_al(at, 16), n), pl.ds(_al(lax.rem(g, SP) * chunk, 128), chunk)]

    def own(st, g):
        h = head_of(g)
        if st == 0:
            n = shard // 4
            rows, at = pl.ds(_al(j * n, 16), n), pl.ds(_al(s * shard + j * n, 16), n)
            return [(wq_ref.at[rows, pl.ds(_al(h * gw, 128), gw)], wl.at[g, at, pl.ds(0, gw)]),
                    (wk_ref.at[rows, pl.ds(_al(h * HEAD, 128), HEAD)], wl.at[g, at, pl.ds(gw, HEAD)]),
                    (wv_ref.at[rows, pl.ds(_al(h * HEAD, 128), HEAD)], wl.at[g, at, pl.ds(gw + HEAD, HEAD)])]
        n = shard_o // 4
        rows = pl.ds(_al(lax.div(g, SP) * shard_o + j * n, 16), n)
        return [(wo_ref.at[rows, pl.ds(_al(lax.rem(g, SP) * chunk, 128), chunk)], piece(1, g, s, j))]

    def to_chip_copy(st, g, i):
        p = piece(st, g, sources[i], j)
        return remote(p, p, sy.at[st, g, i], ry.at[st, g, i], to_chip)

    def to_core_copy(st, g, i):
        p = piece(st, g, sources[i % 3], j if i < 3 else jy)
        return remote(p, p, sc.at[st, g, i], rc.at[st, g, i], to_core)

    def on(st, g, src, device, way):
        part = piece(st, g, src, j, way)
        return remote(part, part, sx2.at[st, g, way], rx2.at[st, g, way], device)

    def arrived(ref, sem):
        remote(ref, ref, sem, sem, to_core).wait_recv()

    def g0(st, g):
        for way, device in ((0, to_right), (1, to_left)):
            for src, dst in own(st, g):
                remote(src, dst, sx.at[st, g, way], rx.at[st, g, way], device).start()

    def g1(st, g):
        for way, src, device in ((0, left, to_right), (1, right, to_left)):
            arrived(piece(st, g, src, j), rx.at[st, g, way])
            on(st, g, src, device, way).start()
            to_chip_copy(st, g, way).start()
            to_core_copy(st, g, way).start()

    def g2(st, g):
        for way in (0, 1):
            arrived(piece(st, g, opp, j, way), rx2.at[st, g, way])
        to_chip_copy(st, g, 2).start()
        to_core_copy(st, g, 2).start()

    def g3(st, g):
        for i in range(3):
            arrived(piece(st, g, sources[i], jy), ry.at[st, g, i])
            to_core_copy(st, g, 3 + i).start()

    def g4(st, g):
        for i in range(6):
            arrived(piece(st, g, sources[i % 3], jc if i < 3 else jcy), rc.at[st, g, i])

    def both(stage, g):
        @pl.when(g < heads)
        def _():
            stage(0, g)

        @pl.when((g >= LAG) & (g < heads + LAG))
        def _():
            stage(1, g - LAG)

    def sent(st, g):
        for way, src, device in ((0, left, to_right), (1, right, to_left)):
            p = piece(st, g, s, j)
            remote(p, p, sx.at[st, g, way], rx.at[st, g, way], device).wait_send()
            on(st, g, src, device, way).wait_send()
        for i in range(3):
            to_chip_copy(st, g, i).wait_send()
        for i in range(6):
            to_core_copy(st, g, i).wait_send()

    def fetches(g):
        h = head_of(g)
        mine = pl.ds(_al(s * shard, 16), shard)
        out = [pltpu.make_async_copy(wq_ref.at[:, pl.ds(_al(h * gw, 128), gw)], w_s.at[mine, pl.ds(0, gw)], fetch.at[0]),
               pltpu.make_async_copy(wk_ref.at[:, pl.ds(_al(h * HEAD, 128), HEAD)], w_s.at[mine, pl.ds(gw, HEAD)], fetch.at[1]),
               pltpu.make_async_copy(wv_ref.at[:, pl.ds(_al(h * HEAD, 128), HEAD)], w_s.at[mine, pl.ds(gw + HEAD, HEAD)], fetch.at[2])]
        for i, src in enumerate(sources):
            at = pl.ds(_al(src * shard, 16), shard)
            out.append(pltpu.make_async_copy(wl.at[g, at, :], w_s.at[at, :], fetch.at[3 + i]))
        return out

    def wo_fetches(half, c, slot):
        at = pl.ds(_al(c * chunk, 128), chunk)
        mine = pl.ds(_al(s * shard_o, 16), shard_o)
        out = [pltpu.make_async_copy(wo_ref.at[pl.ds(_al(half * shard_o, 16), shard_o), at], wo_s.at[slot, mine, :], wfetch.at[slot, 0])]
        for i, src in enumerate(sources):
            rows = pl.ds(_al(src * shard_o, 16), shard_o)
            out.append(pltpu.make_async_copy(wol.at[half, rows, at], wo_s.at[slot, rows, :], wfetch.at[slot, 1 + i]))
        return out

    def project(g):
        slot, par, m = lax.rem(g, SLOTS), lax.rem(g, 2), B

        def tile(i, _):
            rows = pl.ds(_al(i * m, 128), m)
            r = _dot(a_s[rows, :], w_s[...], 1, 0).astype(jnp.bfloat16)
            cos, sin = cos_ref[rows, :], sin_ref[rows, :]

            def turned(t):
                t = t.astype(jnp.float32)
                return (t * cos + pltpu.roll(t, HEAD // 2, 1) * sin).astype(jnp.bfloat16)

            k_s[slot, s, rows, :] = turned(r[:, gw : gw + HEAD])
            v_s[slot, s, :, rows] = r[:, gw + HEAD :].T
            for n in range(group):
                q_s[par, pl.ds(_al(n * tokens + i * m, 128), m), :] = turned(r[:, n * HEAD : (n + 1) * HEAD])

        lax.fori_loop(0, tokens // m, tile, None)

    def kv(g, src, which, number, device):
        slot = lax.rem(g, SLOTS)
        ref = (k_s if which == 0 else v_s).at[slot, src]
        return remote(ref, ref, skv.at[g, number], rkv.at[g, src, which], device)

    own_kv = (
        (lambda: s < 2, 1, 2, to_left),
        (lambda: s == 0, 0, 3, to_left),
        (lambda: s < 3, 0, 0, to_right),
        (lambda: s < 3, 1, 1, to_right),
    )
    passed_on = ((0, 1, 1, to_left), (1, 0, 0, to_right), (2, 1, 0, to_right), (3, 0, 1, to_left))

    def kv_send(g):
        for who, which, number, device in own_kv:
            @pl.when(who())
            def _():
                kv(g, s, which, number, device).start()

    def kv_on(g, copies):
        for place, src, which, device in copies:
            @pl.when(s == place)
            def _():
                copy = kv(g, src, which, 4, device)
                copy.wait_recv()
                copy.start()

    def kv_sent(g):
        for who, which, number, device in own_kv:
            @pl.when(who())
            def _():
                kv(g, s, which, number, device).wait_send()
        for place, src, which, device in passed_on:
            @pl.when(s == place)
            def _():
                kv(g, src, which, 4, device).wait_send()

    e = HEAD**-0.5 * LOG2E

    def block(g, src, kb, strips, first=False, masked=()):
        slot, par = lax.rem(g, SLOTS), lax.rem(g, 2)
        at_k = pl.ds(kb * B if isinstance(kb, int) else _al(kb * B, 128), B)
        k = k_s[slot, src, at_k, :]
        values = jnp.concatenate([v_s[slot, src, :, at_k], jnp.ones((8, B), jnp.bfloat16)], axis=0)
        scores = [_dot(k, q_s[par, at : at + B, :], 1, 1) for at in strips]
        weights, keeps = [], []
        for at, sc_ in zip(strips, scores):
            if at in masked:
                seen = lax.broadcasted_iota(jnp.int32, (B, B), 1) >= lax.broadcasted_iota(jnp.int32, (B, B), 0)
                sc_ = jnp.where(seen, sc_, -1e30)
            top = sc_.max(axis=0, keepdims=True)
            if not first:
                old = top_s[:, at : at + B]
                top = jnp.maximum(old, top)
                keeps.append(jnp.exp2((old - top) * e))
            top_s[:, at : at + B] = top
            weights.append(jnp.exp2((sc_ - top) * e).astype(jnp.bfloat16))
        for n, (at, p) in enumerate(zip(strips, weights)):
            new = _dot(values, p, 1, 0)
            mix_s[:, at : at + B] = new if first else mix_s[:, at : at + B] * keeps[n] + new

    strips = [n * tokens + half * B for n in range(group) for half in (0, 1)]

    def finish(g):
        half, i = lax.div(g, SP), lax.rem(g, SP)
        for n in range(group):
            at = slice(n * tokens, (n + 1) * tokens)
            out = mix_s[:HEAD, at] * (1 / mix_s[HEAD : HEAD + 1, at])
            o_s[half, :, pl.ds(_al(i * gw + n * HEAD, 128), HEAD)] = out.T.astype(jnp.bfloat16)

    barrier = pltpu.get_barrier_semaphore()
    for device in (to_left, to_right, to_core, to_chip):
        pl.semaphore_signal(barrier, inc=1, device_id=device, device_id_type=MESH)
    load = pltpu.make_async_copy(x_ref, a_s, local.at[0])
    load.start()
    pl.semaphore_wait(barrier, 4)
    both(g0, jnp.int32(0))
    load.wait()

    def norm(i, _):
        rows = pl.ds(_al(i * 64, 16), 64)
        wide = a_s[rows, :].astype(jnp.float32)
        acc_s[rows, :] = wide
        scale = lax.rsqrt(jnp.mean(wide * wide, -1, keepdims=True) + 1e-6)
        a_s[rows, :] = (wide * scale * gain_ref[...].astype(jnp.float32)).astype(jnp.bfloat16)

    lax.fori_loop(0, tokens // 64, norm, None)
    def begin(*stages):
        for stage, g in stages:
            both(stage, jnp.int32(g))

    begin((g1, 0), (g0, 1), (g2, 0), (g1, 1), (g0, 2), (g2, 1), (g1, 2), (g0, 3), (g3, 0), (g4, 0))
    for f in fetches(0):
        f.start()
    for f in fetches(0):
        f.wait()
    project(0)
    kv_send(0)
    begin((g2, 2), (g1, 3), (g0, 4), (g3, 1))

    def step(t, _):
        @pl.when(t + 1 < heads)
        def _():
            g4(0, t + 1)
            for f in fetches(t + 1):
                f.start()

        @pl.when(t + 1 >= LAG)
        def _():
            g4(1, t + 1 - LAG)

        @pl.when(t >= SP)
        def _():
            for f in wo_fetches(0, t - SP, 0):
                f.start()

        kv_on(t, passed_on[:3])
        block(t, s, 0, strips, first=True, masked=strips[0::2])
        block(t, s, 1, strips[1::2], masked=strips[1::2])
        kv_on(t, passed_on[3:])

        @pl.when(t + 1 < heads)
        def _():
            for f in fetches(t + 1):
                f.wait()
            project(t + 1)
            kv_send(t + 1)

        both(g0, t + 5)

        def other(i, _):
            src = jnp.where(i == 1, s - 1, i - 2)

            @pl.when(s >= i)
            def _():
                @pl.when((i > 1) | (s == 3))
                def _():
                    kv(t, src, 0, 5, to_left).wait_recv()

                @pl.when((i != 2) | (s != 3))
                def _():
                    kv(t, src, 1, 5, to_left).wait_recv()

                lax.fori_loop(0, 2, lambda kb, _: block(t, src, kb, strips), None)

            for n, stage, ahead in ((1, g1, 4), (2, g2, 3), (3, g3, 2)):
                @pl.when(i == n)
                def _():
                    both(stage, t + ahead)

        lax.fori_loop(1, SP, other, None)
        finish(t)
        kv_sent(t)

        @pl.when(t >= SP)
        def _():
            c = t - SP
            for f in wo_fetches(0, c, 0):
                f.wait()

            def tile(i, _):
                rows, at = pl.ds(_al(i * B, 128), B), pl.ds(_al(c * chunk, 128), chunk)
                acc_s[rows, at] += _dot(o_s[0, rows, :], wo_s[0], 1, 0)

            lax.fori_loop(0, tokens // B, tile, None)

    lax.fori_loop(0, heads, step, None)

    for f in wo_fetches(1, 0, 0):
        f.start()
    g4(1, heads - 1)

    def last(c, _):
        slot = lax.rem(c, 2)

        @pl.when(c + 1 < SP)
        def _():
            for f in wo_fetches(1, c + 1, 1 - slot):
                f.start()

        for f in wo_fetches(1, c, slot):
            f.wait()
        at = pl.ds(_al(c * chunk, 128), chunk)

        def tile(i, _):
            rows = pl.ds(_al(i * B, 128), B)
            a_s[rows, at] = (acc_s[rows, at] + _dot(o_s[1, rows, :], wo_s[slot], 1, 0)).astype(jnp.bfloat16)

        lax.fori_loop(0, tokens // B, tile, None)
        pltpu.make_async_copy(a_s.at[:, at], y_ref.at[:, at], local.at[c]).start()

    lax.fori_loop(0, SP, last, None)

    def drain(g, _):
        sent(0, g)
        sent(1, g)

    lax.fori_loop(0, heads, drain, None)
    for c in range(SP):
        at = pl.ds(c * chunk, chunk)
        pltpu.make_async_copy(a_s.at[:, at], y_ref.at[:, at], local.at[c]).wait()


def solution(mesh):
    def step(x, gain, wq, wk, wv, wo):
        tokens, depth = x.shape
        heads, group = wk.shape[1] // HEAD, wq.shape[1] // wk.shape[1]
        half = HEAD // 2
        place = lax.axis_index("sp") * tokens + jnp.arange(tokens)
        angle = place.astype(jnp.float32)[:, None] * THETA ** (-jnp.arange(half, dtype=jnp.float32) / half)
        cos, sin = jnp.cos(angle), jnp.sin(angle)
        cos, sin = jnp.concatenate([cos, cos], -1), jnp.concatenate([-sin, sin], -1)
        width, B = (group + 2) * HEAD, tokens // 2
        low, wide = jnp.bfloat16, jnp.float32
        half_o = wo.shape[0] // 2 * SP
        anywhere, vmem = pl.BlockSpec(memory_space=pl.ANY), pl.BlockSpec(memory_space=pltpu.VMEM)
        dma = pltpu.SemaphoreType.DMA
        flops = 2 * tokens * depth * (wq.shape[1] * 2 + 2 * wk.shape[1]) + 4 * tokens * tokens * wq.shape[1] * SP
        y, _, _ = pl.pallas_call(
            functools.partial(_kernel, group),
            out_shape=[jax.ShapeDtypeStruct(x.shape, low), jax.ShapeDtypeStruct((heads, depth, width), low),
                       jax.ShapeDtypeStruct((2, half_o, depth), low)],
            in_specs=[anywhere, vmem, vmem, vmem, anywhere, anywhere, anywhere, anywhere],
            out_specs=[anywhere, anywhere, anywhere],
            scratch_shapes=[
                pltpu.VMEM((tokens, depth), low),
                pltpu.VMEM((tokens, depth), wide),
                pltpu.VMEM((2, tokens, half_o), low),
                pltpu.VMEM((SLOTS, SP, tokens, HEAD), low),
                pltpu.VMEM((SLOTS, SP, HEAD, tokens), low),
                pltpu.VMEM((2, group * tokens, HEAD), low),
                pltpu.VMEM((depth, width), low),
                pltpu.VMEM((2, half_o, depth // SP), low),
                pltpu.VMEM((1, group * tokens), wide),
                pltpu.VMEM((HEAD + 8, group * tokens), wide),
                dma((2, heads, 2)), dma((2, heads, 2)), dma((2, heads, 2)), dma((2, heads, 2)),
                dma((2, heads, 3)), dma((2, heads, 3)), dma((2, heads, 6)), dma((2, heads, 6)),
                dma((heads, 6)), dma((heads, SP, 2)), dma((SP,)), dma((6,)), dma((2, SP)),
            ],
            compiler_params=pltpu.CompilerParams(collective_id=0, has_side_effects=True, vmem_limit_bytes=67043328),
            cost_estimate=pl.CostEstimate(flops=flops, transcendentals=tokens * tokens * 2 * heads * group, bytes_accessed=200 * 2**20),
        )(x, gain[None, :], cos, sin, wq, wk, wv, wo)
        return y

    tokens, whole = P(("dp", "sp"), None), P("sp", None)
    return jax.shard_map(
        step,
        mesh=mesh,
        in_specs=(tokens, P(None), whole, whole, whole, whole),
        out_specs=tokens,
        check_vma=False,
    )
```

```python
import functools

import jax
import jax.numpy as jnp
import numpy as np
from jax import lax
from jax.experimental import pallas as pl
from jax.experimental.pallas import tpu as pltpu
from jax.sharding import PartitionSpec as P

HEAD = 128
THETA = 10000
LOG2E = 1.4426950408889634
SP = 4
SLOTS = 6
LAG = 3
MESH = pl.DeviceIdType.MESH


def _dot(a, b, ca, cb):
    return lax.dot_general(a, b, (((ca,), (cb,)), ((), ())), preferred_element_type=jnp.float32)


def _al(i, unit):
    return pl.multiple_of(i, unit)


def _kernel(group, x_ref, gain_ref, freq_ref, wq_ref, wk_ref, wv_ref, wo_ref, o_ref, acc, wl, wol, part,
            a_s, o_s, k_s, v_s, q_s, w_s, part_s, wo_s, wo_c, acc_s, top_s, mix_s, cos_s, sin_s,
            sw, rx, rx2, ry, rc, skv, rkv, local, fetch, pfetch, wo_sem, o_sem, acc_sem):
    tokens, depth = x_ref.shape
    heads = wk_ref.shape[1] // HEAD
    gw = group * HEAD
    width = gw + 2 * HEAD
    shard = depth // SP
    shard_o = wo_ref.shape[0] // 2
    chunk = depth // SP
    B = tokens // 2
    cols = group * tokens

    s, d = lax.axis_index("sp"), lax.axis_index("dp")
    left, right, opp = lax.rem(s + 3, SP), lax.rem(s + 1, SP), lax.rem(s + 2, SP)
    j = lax.rem(d, 4)
    core = lax.rem(j, 2)
    jy = lax.rem(j + 2, 4)
    to_left, to_right = {"sp": left}, {"sp": right}
    to_core = {"dp": d + 1 - 2 * core}
    to_chip = {"dp": d + 2 - 4 * lax.div(j, 2)}
    sources = (left, right, opp)

    def remote(src, dst, send, recv, device):
        return pltpu.make_async_remote_copy(src_ref=src, dst_ref=dst, send_sem=send, recv_sem=recv, device_id=device, device_id_type=MESH)

    def head_of(g):
        return 2 * lax.rem(g, SP) + lax.div(g, SP)

    def piece(st, g, src, jj, part=None):
        if st == 0:
            n = shard // 4
            at, n = (src * shard + jj * n, n) if part is None else (src * shard + jj * n + part * (n // 2), n // 2)
            return wl.at[g, pl.ds(_al(at, 16), n), :]
        n = shard_o // 4
        at, n = (src * shard_o + jj * n, n) if part is None else (src * shard_o + jj * n + part * (n // 2), n // 2)
        return wol.at[lax.div(g, SP), pl.ds(_al(at, 16), n), pl.ds(_al(lax.rem(g, SP) * chunk, 128), chunk)]

    def own(st, g):
        h = head_of(g)
        if st == 0:
            n = shard // 4
            rows, at = pl.ds(_al(j * n, 16), n), pl.ds(_al(s * shard + j * n, 16), n)
            return [(wq_ref.at[rows, pl.ds(_al(h * gw, 128), gw)], wl.at[g, at, pl.ds(0, gw)]),
                    (wk_ref.at[rows, pl.ds(_al(h * HEAD, 128), HEAD)], wl.at[g, at, pl.ds(gw, HEAD)]),
                    (wv_ref.at[rows, pl.ds(_al(h * HEAD, 128), HEAD)], wl.at[g, at, pl.ds(gw + HEAD, HEAD)])]
        n = shard_o // 4
        rows = pl.ds(_al(lax.div(g, SP) * shard_o + j * n, 16), n)
        return [(wo_ref.at[rows, pl.ds(_al(lax.rem(g, SP) * chunk, 128), chunk)], piece(1, g, s, j))]

    def to_chip_copy(st, g, i):
        p = piece(st, g, sources[i], j)
        return remote(p, p, sw.at[st, g], ry.at[st, g], to_chip)

    def to_core_copy(st, g, i):
        p = piece(st, g, sources[i % 3], j if i < 3 else jy)
        return remote(p, p, sw.at[st, g], rc.at[st, g], to_core)

    def on(st, g, src, device, way):
        part = piece(st, g, src, j, way)
        return remote(part, part, sw.at[st, g], rx2.at[st, g], device)

    def arrived(ref, sem):
        remote(ref, ref, sem, sem, to_core).wait_recv()

    def pieces(st, g, n):
        if st == 0:
            return wl.at[g, pl.ds(0, n * (shard // 4)), :]
        return wol.at[lax.div(g, SP), pl.ds(0, n * (shard_o // 4)), pl.ds(_al(lax.rem(g, SP) * chunk, 128), chunk)]

    def g0(st, g):
        for way, device in ((0, to_right), (1, to_left)):
            for src, dst in own(st, g):
                remote(src, dst, sw.at[st, g], rx.at[st, g, way], device).start()

    def g1(st, g):
        for way, src, device in ((0, left, to_right), (1, right, to_left)):
            arrived(piece(st, g, src, j), rx.at[st, g, way])
            on(st, g, src, device, way).start()
            to_chip_copy(st, g, way).start()
            to_core_copy(st, g, way).start()

    def g2(st, g):
        arrived(pieces(st, g, 1), rx2.at[st, g])
        to_chip_copy(st, g, 2).start()
        to_core_copy(st, g, 2).start()

    def g3(st, g):
        arrived(pieces(st, g, 3), ry.at[st, g])
        for i in range(3):
            to_core_copy(st, g, 3 + i).start()

    def g4(st, g):
        arrived(pieces(st, g, 6), rc.at[st, g])

    def both(stage, g):
        @pl.when(g < heads)
        def _():
            stage(0, g)

        @pl.when((g >= LAG) & (g < heads + LAG))
        def _():
            stage(1, g - LAG)

    def sent(st, g):
        all_of = pieces(st, g, 12)
        remote(all_of, all_of, sw.at[st, g], rx2.at[st, g], to_core).wait_send()

    def own_fetches(g):
        h, par = head_of(g), lax.rem(g, 2)
        rows = pl.ds(_al(par * shard, 16), shard)
        return [pltpu.make_async_copy(wq_ref.at[:, pl.ds(_al(h * gw, 128), gw)], w_s.at[rows, pl.ds(0, gw)], pfetch.at[par, 0]),
                pltpu.make_async_copy(wk_ref.at[:, pl.ds(_al(h * HEAD, 128), HEAD)], w_s.at[rows, pl.ds(gw, HEAD)], pfetch.at[par, 1]),
                pltpu.make_async_copy(wv_ref.at[:, pl.ds(_al(h * HEAD, 128), HEAD)], w_s.at[rows, pl.ds(gw + HEAD, HEAD)], pfetch.at[par, 2])]

    def part_copy(g, i):
        return pltpu.make_async_copy(part_s.at[i], part.at[g, i], local.at[i])

    def own_parts(first, end):
        def one(g, _):
            @pl.when(g + 1 < heads)
            def _():
                for f in own_fetches(g + 1):
                    f.start()

            for f in own_fetches(g):
                f.wait()
            rows = pl.ds(_al(lax.rem(g, 2) * shard, 16), shard)

            def tile(i, _):
                @pl.when(g > 0)
                def _():
                    part_copy(g - 1, i).wait()

                part_s[i] = _dot(a_s[pl.ds(_al(i * B, 128), B), :shard], w_s[rows, :], 1, 0)
                part_copy(g, i).start()

            lax.fori_loop(0, 2, tile, None)

        lax.fori_loop(first, end, one, None)

    def fetches(g):
        out = [pltpu.make_async_copy(wl.at[g, pl.ds(_al(src * shard, 16), shard), :], w_s.at[pl.ds(i * shard, shard), :], fetch.at[i])
               for i, src in enumerate(sources)]
        return out + [pltpu.make_async_copy(part.at[g, i], part_s.at[i], fetch.at[3 + i]) for i in (0, 1)]

    def wo_in(half):
        return pltpu.make_async_copy(wo_ref.at[pl.ds(half * shard_o, shard_o), :], wo_s.at[half], wo_sem.at[half])

    def wo_out(half):
        return pltpu.make_async_copy(wo_s.at[half], wol.at[half, pl.ds(_al(s * shard_o, 16), shard_o), :], wo_sem.at[half])

    def o_out(g):
        at = pl.ds(_al(lax.rem(g, SP) * gw, 128), gw)
        return pltpu.make_async_copy(o_s.at[1, :, at], o_ref.at[:, at], o_sem.at[lax.rem(g, SP)])

    def wo_chunk(c):
        return pltpu.make_async_copy(wol.at[0, :, pl.ds(_al(c * chunk, 128), chunk)], wo_c, acc_sem.at[0])

    def acc_out(c):
        return pltpu.make_async_copy(acc_s, acc.at[:, pl.ds(_al(c * chunk, 128), chunk)], acc_sem.at[1])

    def project(g):
        slot, par, m = lax.rem(g, SLOTS), lax.rem(g, 2), B

        def tile(i, _):
            rows = pl.ds(_al(i * m, 128), m)
            r = (part_s[i] + _dot(a_s[rows, shard:], w_s[...], 1, 0)).astype(jnp.bfloat16)
            cos, sin = cos_s[rows, :], sin_s[rows, :]

            def turned(t):
                t = t.astype(jnp.float32)
                return (t * cos + pltpu.roll(t, HEAD // 2, 1) * sin).astype(jnp.bfloat16)

            k_s[slot, s, rows, :] = turned(r[:, gw : gw + HEAD])
            v_s[slot, s, :, rows] = r[:, gw + HEAD :].T
            for n in range(group):
                q_s[par, pl.ds(_al(n * tokens + i * m, 128), m), :] = turned(r[:, n * HEAD : (n + 1) * HEAD])

        lax.fori_loop(0, tokens // m, tile, None)

    def kv(g, src, which, number, device):
        slot = lax.rem(g, SLOTS)
        ref = (k_s if which == 0 else v_s).at[slot, src]
        return remote(ref, ref, skv.at[g, number], rkv.at[g, src, which], device)

    own_kv = (
        (lambda: s < 2, 1, 2, to_left),
        (lambda: s == 0, 0, 3, to_left),
        (lambda: s < 3, 0, 0, to_right),
        (lambda: s < 3, 1, 1, to_right),
    )
    passed_on = ((0, 1, 1, to_left), (1, 0, 0, to_right), (2, 1, 0, to_right), (3, 0, 1, to_left))

    def kv_send(g):
        for who, which, number, device in own_kv:
            @pl.when(who())
            def _():
                kv(g, s, which, number, device).start()

    def kv_on(g, copies):
        for place, src, which, device in copies:
            @pl.when(s == place)
            def _():
                copy = kv(g, src, which, 4, device)
                copy.wait_recv()
                copy.start()

    def kv_sent(g):
        for who, which, number, device in own_kv:
            @pl.when(who())
            def _():
                kv(g, s, which, number, device).wait_send()
        for place, src, which, device in passed_on:
            @pl.when(s == place)
            def _():
                kv(g, src, which, 4, device).wait_send()

    e = HEAD**-0.5 * LOG2E

    def block(g, src, kb, strips, first=False, masked=()):
        slot, par = lax.rem(g, SLOTS), lax.rem(g, 2)
        at_k = pl.ds(kb * B if isinstance(kb, int) else _al(kb * B, 128), B)
        k = k_s[slot, src, at_k, :]
        values = jnp.concatenate([v_s[slot, src, :, at_k], jnp.ones((8, B), jnp.bfloat16)], axis=0)
        scores = [_dot(k, q_s[par, at : at + B, :], 1, 1) for at in strips]
        weights, keeps = [], []
        for at, sc_ in zip(strips, scores):
            if at in masked:
                seen = lax.broadcasted_iota(jnp.int32, (B, B), 1) >= lax.broadcasted_iota(jnp.int32, (B, B), 0)
                sc_ = jnp.where(seen, sc_, -1e30)
            top = sc_.max(axis=0, keepdims=True)
            if not first:
                old = top_s[:, at : at + B]
                top = jnp.maximum(old, top)
                keeps.append(jnp.exp2((old - top) * e))
            top_s[:, at : at + B] = top
            weights.append(jnp.exp2((sc_ - top) * e).astype(jnp.bfloat16))
        for n, (at, p) in enumerate(zip(strips, weights)):
            new = _dot(values, p, 1, 0)
            mix_s[:, at : at + B] = new if first else mix_s[:, at : at + B] * keeps[n] + new

    strips = [n * tokens + half * B for n in range(group) for half in (0, 1)]

    def finish(g):
        half, i = lax.div(g, SP), lax.rem(g, SP)
        for n in range(group):
            at = slice(n * tokens, (n + 1) * tokens)
            out = mix_s[:HEAD, at] * (1 / mix_s[HEAD : HEAD + 1, at])
            o_s[half, :, pl.ds(_al(i * gw + n * HEAD, 128), HEAD)] = out.T.astype(jnp.bfloat16)

    barrier = pltpu.get_barrier_semaphore()
    for device in (to_left, to_right, to_core, to_chip):
        pl.semaphore_signal(barrier, inc=1, device_id=device, device_id_type=MESH)
    columns = [(pl.ds(_al(src * shard, 128), shard), slice(i * shard, (i + 1) * shard)) for i, src in enumerate((s, *sources))]
    loads = [pltpu.make_async_copy(x_ref.at[:, at], a_s.at[:, to], local.at[i]) for i, (at, to) in enumerate(columns)]
    for f in [*loads, *own_fetches(jnp.int32(0)), wo_in(0), wo_in(1)]:
        f.start()
    pl.semaphore_wait(barrier, 4)
    both(g0, jnp.int32(0))
    for f in loads:
        f.wait()

    def norm(i, _):
        rows = pl.ds(_al(i * 64, 16), 64)
        wide = a_s[rows, :].astype(jnp.float32)
        scale = lax.rsqrt(jnp.mean(wide * wide, -1, keepdims=True) + 1e-6)
        gain = jnp.concatenate([gain_ref[:, at] for at, _ in columns], axis=1).astype(jnp.float32)
        a_s[rows, :] = (wide * scale * gain).astype(jnp.bfloat16)

    lax.fori_loop(0, tokens // 64, norm, None)

    def begin(*stages):
        for stage, g in stages:
            both(stage, jnp.int32(g))

    def turns(i, _):
        rows = pl.ds(_al(i * 64, 16), 64)
        place = s * tokens + i * 64 + lax.broadcasted_iota(jnp.int32, (64, HEAD), 0)
        angle = place.astype(jnp.float32) * freq_ref[...]
        sin = jnp.sin(angle)
        cos_s[rows, :] = jnp.cos(angle)
        sin_s[rows, :] = jnp.where(lax.broadcasted_iota(jnp.int32, (64, HEAD), 1) < HEAD // 2, -sin, sin)

    begin((g1, 0), (g0, 1))
    own_parts(0, 2)
    begin((g2, 0), (g1, 1), (g0, 2))
    own_parts(2, 6)
    begin((g2, 1), (g3, 0), (g0, 3))
    own_parts(6, heads)
    lax.fori_loop(0, tokens // 64, turns, None)
    for i in (0, 1):
        part_copy(heads - 1, i).wait()
    for half in (0, 1):
        wo_in(half).wait()
        wo_out(half).start()
    begin((g4, 0))
    for f in fetches(0):
        f.start()
    for f in fetches(0):
        f.wait()
    project(0)
    kv_send(0)
    begin((g1, 2), (g2, 2), (g1, 3), (g0, 4), (g3, 1))

    def step(t, _):
        @pl.when(t + 1 < heads)
        def _():
            g4(0, t + 1)
            for f in fetches(t + 1):
                f.start()

        @pl.when(t + 1 >= LAG)
        def _():
            g4(1, t + 1 - LAG)

        @pl.when(t == SP)
        def _():
            for half in (0, 1):
                wo_out(half).wait()

        @pl.when(t >= SP)
        def _():
            wo_chunk(t - SP).start()

        kv_on(t, passed_on[:3])
        block(t, s, 0, strips, first=True, masked=strips[0::2])
        block(t, s, 1, strips[1::2], masked=strips[1::2])
        kv_on(t, passed_on[3:])

        @pl.when(t + 1 < heads)
        def _():
            for f in fetches(t + 1):
                f.wait()
            project(t + 1)
            kv_send(t + 1)

        both(g0, t + 5)

        @pl.when(t >= SP)
        def _():
            c = t - SP
            wo_chunk(c).wait()

            @pl.when(c > 0)
            def _():
                acc_out(c - 1).wait()

            def tile(i, _):
                rows = pl.ds(_al(i * B, 128), B)
                acc_s[rows, :] = _dot(o_s[0, rows, :], wo_c[...], 1, 0)

            lax.fori_loop(0, tokens // B, tile, None)
            acc_out(c).start()


        def other(i, _):
            src = jnp.where(i == 1, s - 1, i - 2)

            @pl.when(s >= i)
            def _():
                @pl.when((i > 1) | (s == 3))
                def _():
                    kv(t, src, 0, 5, to_left).wait_recv()

                @pl.when((i != 2) | (s != 3))
                def _():
                    kv(t, src, 1, 5, to_left).wait_recv()

                block(t, src, 0, strips)
                block(t, src, 1, strips)

            for n, stage, ahead in ((1, g3, 2), (2, g2, 3), (3, g1, 4)):
                @pl.when(i == n)
                def _():
                    both(stage, t + ahead)

        lax.fori_loop(1, SP, other, None)
        finish(t)
        kv_sent(t)
        both(sent, t)

        @pl.when(t >= SP)
        def _():
            o_out(t).start()

    lax.fori_loop(0, heads, step, None)

    for g in range(heads + LAG - 2, heads + LAG):
        if g > heads + 1:
            g3(1, g - LAG)
        g4(1, g - LAG)
    acc_out(SP - 1).wait()
    for g in range(heads - SP, heads):
        o_out(jnp.int32(g)).wait()
    for g in range(heads, heads + LAG):
        sent(1, g - LAG)


def _project_out(x_ref, acc_ref, o_ref, w_ref, y_ref):
    tokens = x_ref.shape[0]
    for m in range(0, tokens, tokens // 2):
        rows = slice(m, m + tokens // 2)
        y_ref[rows, :] = (x_ref[rows, :].astype(jnp.float32) + acc_ref[rows, :] + _dot(o_ref[rows, :], w_ref[0], 1, 0)).astype(jnp.bfloat16)


def solution(mesh):
    def step(x, gain, wq, wk, wv, wo):
        tokens, depth = x.shape
        heads, group = wk.shape[1] // HEAD, wq.shape[1] // wk.shape[1]
        freq = np.float32(THETA) ** (-np.arange(HEAD // 2, dtype=np.float32) / np.float32(HEAD // 2))
        freq = np.concatenate([freq, freq])[None, :]
        width, B = (group + 2) * HEAD, tokens // 2
        low, wide = jnp.bfloat16, jnp.float32
        half_o = wo.shape[0] // 2 * SP
        anywhere, vmem = pl.BlockSpec(memory_space=pl.ANY), pl.BlockSpec(memory_space=pltpu.VMEM)
        dma = pltpu.SemaphoreType.DMA
        flops = 2 * tokens * depth * (wq.shape[1] * 2 + 2 * wk.shape[1]) + 4 * tokens * tokens * wq.shape[1] * SP
        seen, acc, _, wo, _ = pl.pallas_call(
            functools.partial(_kernel, group),
            out_shape=[jax.ShapeDtypeStruct((tokens, half_o), low), jax.ShapeDtypeStruct(x.shape, wide), jax.ShapeDtypeStruct((heads, depth, width), low),
                       jax.ShapeDtypeStruct((2, half_o, depth), low), jax.ShapeDtypeStruct((heads, 2, B, width), wide)],
            in_specs=[anywhere, vmem, vmem, anywhere, anywhere, anywhere, anywhere],
            out_specs=[anywhere] * 5,
            scratch_shapes=[
                pltpu.VMEM((tokens, depth), low),
                pltpu.VMEM((2, tokens, half_o), low),
                pltpu.VMEM((SLOTS, SP, tokens, HEAD), low),
                pltpu.VMEM((SLOTS, SP, HEAD, tokens), low),
                pltpu.VMEM((2, group * tokens, HEAD), low),
                pltpu.VMEM((depth - depth // SP, width), low),
                pltpu.VMEM((2, B, width), wide),
                pltpu.VMEM((2, wo.shape[0] // 2, depth), low),
                pltpu.VMEM((half_o, depth // SP), low),
                pltpu.VMEM((tokens, depth // SP), wide),
                pltpu.VMEM((1, group * tokens), wide),
                pltpu.VMEM((HEAD + 8, group * tokens), wide),
                pltpu.VMEM((tokens, HEAD), wide),
                pltpu.VMEM((tokens, HEAD), wide),
                dma((2, heads)), dma((2, heads, 2)), dma((2, heads)), dma((2, heads)), dma((2, heads)),
                dma((heads, 6)), dma((heads, SP, 2)), dma((SP,)), dma((5,)), dma((2, 3)), dma((2,)), dma((SP,)), dma((2,)),
            ],
            compiler_params=pltpu.CompilerParams(collective_id=0, has_side_effects=True, vmem_limit_bytes=67043328),
            cost_estimate=pl.CostEstimate(flops=flops, transcendentals=tokens * tokens * 2 * heads * group, bytes_accessed=200 * 2**20),
        )(x, gain[None, :], freq, wq, wk, wv, wo)
        n = depth // 6
        return pl.pallas_call(
            _project_out,
            out_shape=jax.ShapeDtypeStruct(x.shape, low),
            grid=(depth // n,),
            in_specs=[pl.BlockSpec((tokens, n), lambda i: (0, i)), pl.BlockSpec((tokens, n), lambda i: (0, i)),
                      pl.BlockSpec((tokens, half_o), lambda i: (0, 0)), pl.BlockSpec((1, half_o, n), lambda i: (1, 0, i))],
            out_specs=pl.BlockSpec((tokens, n), lambda i: (0, i)),
            compiler_params=pltpu.CompilerParams(dimension_semantics=("arbitrary",), vmem_limit_bytes=60 * 2**20),
            cost_estimate=pl.CostEstimate(flops=2 * tokens * half_o * depth, transcendentals=0, bytes_accessed=40 * 2**20),
        )(x, acc, seen, wo)

    tokens, whole = P(("dp", "sp"), None), P("sp", None)
    return jax.shard_map(
        step,
        mesh=mesh,
        in_specs=(tokens, P(None), whole, whole, whole, whole),
        out_specs=tokens,
        check_vma=False,
    )
```

```python
import functools

import jax
import jax.numpy as jnp
import numpy as np
from jax import lax
from jax.experimental import pallas as pl
from jax.experimental.pallas import tpu as pltpu
from jax.sharding import PartitionSpec as P

HEAD = 128
THETA = 10000
LOG2E = 1.4426950408889634
SP = 4
SLOTS = 6
LAG = 3
MESH = pl.DeviceIdType.MESH


def _dot(a, b, ca, cb):
    return lax.dot_general(a, b, (((ca,), (cb,)), ((), ())), preferred_element_type=jnp.float32)


def _al(i, unit):
    return pl.multiple_of(i, unit)


def _kernel(group, x_ref, gain_ref, freq_ref, wq_ref, wk_ref, wv_ref, wo_ref, o_ref, acc, wl, wol, part,
            a_s, o_s, k_s, v_s, q_s, w_s, part_s, wo_s, wo_c, acc_s, top_s, mix_s, cos_s, sin_s,
            sw, rx, rx2, ry, rc, skv, rkv, local, fetch, pfetch, wo_sem, o_sem, acc_sem):
    tokens, depth = x_ref.shape
    heads = wk_ref.shape[1] // HEAD
    gw = group * HEAD
    width = gw + 2 * HEAD
    shard = depth // SP
    shard_o = wo_ref.shape[0] // 2
    chunk = depth // SP
    B = tokens // 2
    cols = group * tokens

    s, d = lax.axis_index("sp"), lax.axis_index("dp")
    left, right, opp = lax.rem(s + 3, SP), lax.rem(s + 1, SP), lax.rem(s + 2, SP)
    j = lax.rem(d, 4)
    core = lax.rem(j, 2)
    jy = lax.rem(j + 2, 4)
    to_left, to_right = {"sp": left}, {"sp": right}
    to_core = {"dp": d + 1 - 2 * core}
    to_chip = {"dp": d + 2 - 4 * lax.div(j, 2)}
    sources = (left, right, opp)

    def remote(src, dst, send, recv, device):
        return pltpu.make_async_remote_copy(src_ref=src, dst_ref=dst, send_sem=send, recv_sem=recv, device_id=device, device_id_type=MESH)

    def head_of(g):
        return 2 * lax.rem(g, SP) + lax.div(g, SP)

    def piece(st, g, src, jj, part=None):
        if st == 0:
            n = shard // 4
            at, n = (src * shard + jj * n, n) if part is None else (src * shard + jj * n + part * (n // 2), n // 2)
            return wl.at[g, pl.ds(_al(at, 16), n), :]
        n = shard_o // 4
        at, n = (src * shard_o + jj * n, n) if part is None else (src * shard_o + jj * n + part * (n // 2), n // 2)
        return wol.at[lax.div(g, SP), pl.ds(_al(at, 16), n), pl.ds(_al(lax.rem(g, SP) * chunk, 128), chunk)]

    def own(st, g):
        h = head_of(g)
        if st == 0:
            n = shard // 4
            rows, at = pl.ds(_al(j * n, 16), n), pl.ds(_al(s * shard + j * n, 16), n)
            return [(wq_ref.at[rows, pl.ds(_al(h * gw, 128), gw)], wl.at[g, at, pl.ds(0, gw)]),
                    (wk_ref.at[rows, pl.ds(_al(h * HEAD, 128), HEAD)], wl.at[g, at, pl.ds(gw, HEAD)]),
                    (wv_ref.at[rows, pl.ds(_al(h * HEAD, 128), HEAD)], wl.at[g, at, pl.ds(gw + HEAD, HEAD)])]
        n = shard_o // 4
        rows = pl.ds(_al(lax.div(g, SP) * shard_o + j * n, 16), n)
        return [(wo_ref.at[rows, pl.ds(_al(lax.rem(g, SP) * chunk, 128), chunk)], piece(1, g, s, j))]

    def to_chip_copy(st, g, i):
        p = piece(st, g, sources[i], j)
        return remote(p, p, sw.at[st, g], ry.at[st, g], to_chip)

    def to_core_copy(st, g, i):
        p = piece(st, g, sources[i % 3], j if i < 3 else jy)
        return remote(p, p, sw.at[st, g], rc.at[st, g], to_core)

    def on(st, g, src, device, way):
        part = piece(st, g, src, j, way)
        return remote(part, part, sw.at[st, g], rx2.at[st, g], device)

    def arrived(ref, sem):
        remote(ref, ref, sem, sem, to_core).wait_recv()

    def pieces(st, g, n):
        if st == 0:
            return wl.at[g, pl.ds(0, n * (shard // 4)), :]
        return wol.at[lax.div(g, SP), pl.ds(0, n * (shard_o // 4)), pl.ds(_al(lax.rem(g, SP) * chunk, 128), chunk)]

    def g0(st, g):
        for way, device in ((0, to_right), (1, to_left)):
            for src, dst in own(st, g):
                remote(src, dst, sw.at[st, g], rx.at[st, g, way], device).start()

    def g1(st, g):
        for way, src, device in ((0, left, to_right), (1, right, to_left)):
            arrived(piece(st, g, src, j), rx.at[st, g, way])
            on(st, g, src, device, way).start()
            to_chip_copy(st, g, way).start()
            to_core_copy(st, g, way).start()

    def g2(st, g):
        arrived(pieces(st, g, 1), rx2.at[st, g])
        to_chip_copy(st, g, 2).start()
        to_core_copy(st, g, 2).start()

    def g3(st, g):
        arrived(pieces(st, g, 3), ry.at[st, g])
        for i in range(3):
            to_core_copy(st, g, 3 + i).start()

    def g4(st, g):
        arrived(pieces(st, g, 6), rc.at[st, g])

    def both(stage, g):
        @pl.when(g < heads)
        def _():
            stage(0, g)

        @pl.when((g >= LAG) & (g < heads + LAG))
        def _():
            stage(1, g - LAG)

    def sent(st, g):
        all_of = pieces(st, g, 12)
        remote(all_of, all_of, sw.at[st, g], rx2.at[st, g], to_core).wait_send()

    def own_fetches(g):
        h, par = head_of(g), lax.rem(g, 2)
        rows = pl.ds(_al(par * shard, 16), shard)
        return [pltpu.make_async_copy(wq_ref.at[:, pl.ds(_al(h * gw, 128), gw)], w_s.at[rows, pl.ds(0, gw)], pfetch.at[par, 0]),
                pltpu.make_async_copy(wk_ref.at[:, pl.ds(_al(h * HEAD, 128), HEAD)], w_s.at[rows, pl.ds(gw, HEAD)], pfetch.at[par, 1]),
                pltpu.make_async_copy(wv_ref.at[:, pl.ds(_al(h * HEAD, 128), HEAD)], w_s.at[rows, pl.ds(gw + HEAD, HEAD)], pfetch.at[par, 2])]

    def part_copy(g, i):
        return pltpu.make_async_copy(part_s.at[i], part.at[g, i], local.at[i])

    def own_parts(first, end):
        def one(g, _):
            @pl.when(g + 1 < heads)
            def _():
                for f in own_fetches(g + 1):
                    f.start()

            for f in own_fetches(g):
                f.wait()
            rows = pl.ds(_al(lax.rem(g, 2) * shard, 16), shard)

            def tile(i, _):
                @pl.when(g > 0)
                def _():
                    part_copy(g - 1, i).wait()

                part_s[i] = _dot(a_s[pl.ds(_al(i * B, 128), B), :shard], w_s[rows, :], 1, 0)
                part_copy(g, i).start()

            lax.fori_loop(0, 2, tile, None)

        lax.fori_loop(first, end, one, None)

    def fetches(g):
        out = [pltpu.make_async_copy(wl.at[g, pl.ds(_al(src * shard, 16), shard), :], w_s.at[pl.ds(i * shard, shard), :], fetch.at[i])
               for i, src in enumerate(sources)]
        return out + [pltpu.make_async_copy(part.at[g, i], part_s.at[i], fetch.at[3 + i]) for i in (0, 1)]

    def wo_in(half):
        return pltpu.make_async_copy(wo_ref.at[pl.ds(half * shard_o, shard_o), :], wo_s.at[half], wo_sem.at[half])

    def wo_out(half):
        return pltpu.make_async_copy(wo_s.at[half], wol.at[half, pl.ds(_al(s * shard_o, 16), shard_o), :], wo_sem.at[half])

    def o_out(g):
        at = pl.ds(_al(lax.rem(g, SP) * gw, 128), gw)
        return pltpu.make_async_copy(o_s.at[1, :, at], o_ref.at[:, at], o_sem.at[lax.rem(g, SP)])

    def wo_chunk(c):
        return pltpu.make_async_copy(wol.at[0, :, pl.ds(_al(c * chunk, 128), chunk)], wo_c, acc_sem.at[0])

    def acc_out(c):
        return pltpu.make_async_copy(acc_s, acc.at[:, pl.ds(_al(c * chunk, 128), chunk)], acc_sem.at[1])

    def project(g):
        slot, par, m = lax.rem(g, SLOTS), lax.rem(g, 2), B

        def tile(i, _):
            rows = pl.ds(_al(i * m, 128), m)
            r = (part_s[i] + _dot(a_s[rows, shard:], w_s[...], 1, 0)).astype(jnp.bfloat16)
            cos, sin = cos_s[rows, :], sin_s[rows, :]

            def turned(t):
                t = t.astype(jnp.float32)
                return (t * cos + pltpu.roll(t, HEAD // 2, 1) * sin).astype(jnp.bfloat16)

            k_s[slot, s, rows, :] = turned(r[:, gw : gw + HEAD])
            v_s[slot, s, :, rows] = r[:, gw + HEAD :].T
            for n in range(group):
                q_s[par, pl.ds(_al(n * tokens + i * m, 128), m), :] = turned(r[:, n * HEAD : (n + 1) * HEAD])

        lax.fori_loop(0, tokens // m, tile, None)

    def kv(g, src, which, number, device):
        slot = lax.rem(g, SLOTS)
        ref = (k_s if which == 0 else v_s).at[slot, src]
        return remote(ref, ref, skv.at[g, number], rkv.at[g, src, which], device)

    own_kv = (
        (lambda: s < 2, 1, 2, to_left),
        (lambda: s == 0, 0, 3, to_left),
        (lambda: s < 3, 0, 0, to_right),
        (lambda: s < 3, 1, 1, to_right),
    )
    passed_on = ((0, 1, 1, to_left), (1, 0, 0, to_right), (2, 1, 0, to_right), (3, 0, 1, to_left))

    def kv_send(g):
        for who, which, number, device in own_kv:
            @pl.when(who())
            def _():
                kv(g, s, which, number, device).start()

    def kv_on(g, copies):
        for place, src, which, device in copies:
            @pl.when(s == place)
            def _():
                copy = kv(g, src, which, 4, device)
                copy.wait_recv()
                copy.start()

    def kv_sent(g):
        for who, which, number, device in own_kv:
            @pl.when(who())
            def _():
                kv(g, s, which, number, device).wait_send()
        for place, src, which, device in passed_on:
            @pl.when(s == place)
            def _():
                kv(g, src, which, 4, device).wait_send()

    e = HEAD**-0.5 * LOG2E

    def block(g, src, kb, strips, first=False, masked=()):
        slot, par = lax.rem(g, SLOTS), lax.rem(g, 2)
        at_k = pl.ds(kb * B if isinstance(kb, int) else _al(kb * B, 128), B)
        k = k_s[slot, src, at_k, :]
        values = jnp.concatenate([v_s[slot, src, :, at_k], jnp.ones((8, B), jnp.bfloat16)], axis=0)
        scores = [_dot(k, q_s[par, at : at + B, :], 1, 1) for at in strips]
        weights, keeps = [], []
        for at, sc_ in zip(strips, scores):
            if at in masked:
                seen = lax.broadcasted_iota(jnp.int32, (B, B), 1) >= lax.broadcasted_iota(jnp.int32, (B, B), 0)
                sc_ = jnp.where(seen, sc_, -1e30)
            top = sc_.max(axis=0, keepdims=True)
            if not first:
                old = top_s[:, at : at + B]
                top = jnp.maximum(old, top)
                keeps.append(jnp.exp2((old - top) * e))
            top_s[:, at : at + B] = top
            weights.append(jnp.exp2((sc_ - top) * e).astype(jnp.bfloat16))
        for n, (at, p) in enumerate(zip(strips, weights)):
            new = _dot(values, p, 1, 0)
            mix_s[:, at : at + B] = new if first else mix_s[:, at : at + B] * keeps[n] + new

    strips = [n * tokens + half * B for n in range(group) for half in (0, 1)]

    def finish(g):
        half, i = lax.div(g, SP), lax.rem(g, SP)
        for n in range(group):
            at = slice(n * tokens, (n + 1) * tokens)
            out = mix_s[:HEAD, at] * (1 / mix_s[HEAD : HEAD + 1, at])
            o_s[half, :, pl.ds(_al(i * gw + n * HEAD, 128), HEAD)] = out.T.astype(jnp.bfloat16)

    barrier = pltpu.get_barrier_semaphore()
    for device in (to_left, to_right, to_core, to_chip):
        pl.semaphore_signal(barrier, inc=1, device_id=device, device_id_type=MESH)
    columns = [(pl.ds(_al(src * shard, 128), shard), slice(i * shard, (i + 1) * shard)) for i, src in enumerate((s, *sources))]
    loads = [pltpu.make_async_copy(x_ref.at[:, at], a_s.at[:, to], local.at[i]) for i, (at, to) in enumerate(columns)]
    for f in [*loads, *own_fetches(jnp.int32(0)), wo_in(0), wo_in(1)]:
        f.start()
    pl.semaphore_wait(barrier, 4)
    both(g0, jnp.int32(0))
    for f in loads:
        f.wait()

    def norm(i, _):
        rows = pl.ds(_al(i * 64, 16), 64)
        wide = a_s[rows, :].astype(jnp.float32)
        scale = lax.rsqrt(jnp.mean(wide * wide, -1, keepdims=True) + 1e-6)
        gain = jnp.concatenate([gain_ref[at] for at, _ in columns], axis=0).astype(jnp.float32)[None, :]
        a_s[rows, :] = (wide * scale * gain).astype(jnp.bfloat16)

    lax.fori_loop(0, tokens // 64, norm, None)

    def begin(*stages):
        for stage, g in stages:
            both(stage, jnp.int32(g))

    def turns(i, _):
        rows = pl.ds(_al(i * 64, 16), 64)
        place = s * tokens + i * 64 + lax.broadcasted_iota(jnp.int32, (64, HEAD), 0)
        angle = place.astype(jnp.float32) * freq_ref[...]
        sin = jnp.sin(angle)
        cos_s[rows, :] = jnp.cos(angle)
        sin_s[rows, :] = jnp.where(lax.broadcasted_iota(jnp.int32, (64, HEAD), 1) < HEAD // 2, -sin, sin)

    begin((g1, 0), (g0, 1))
    own_parts(0, 2)
    begin((g2, 0), (g1, 1), (g0, 2))
    own_parts(2, 6)
    begin((g2, 1), (g3, 0), (g0, 3))
    own_parts(6, heads)
    lax.fori_loop(0, tokens // 64, turns, None)
    for i in (0, 1):
        part_copy(heads - 1, i).wait()
    begin((g4, 0))
    for f in fetches(0):
        f.start()
    for f in fetches(0):
        f.wait()
    project(0)
    kv_send(0)
    for half in (0, 1):
        wo_in(half).wait()
        wo_out(half).start()
    begin((g1, 2), (g2, 2), (g1, 3), (g0, 4), (g3, 1))

    def step(t, _):
        @pl.when(t + 1 < heads)
        def _():
            g4(0, t + 1)
            for f in fetches(t + 1):
                f.start()

        @pl.when(t + 1 >= LAG)
        def _():
            g4(1, t + 1 - LAG)

        @pl.when(t == SP)
        def _():
            for half in (0, 1):
                wo_out(half).wait()

        @pl.when(t >= SP)
        def _():
            wo_chunk(t - SP).start()

        kv_on(t, passed_on[:3])
        block(t, s, 0, strips, first=True, masked=strips[0::2])
        block(t, s, 1, strips[1::2], masked=strips[1::2])
        kv_on(t, passed_on[3:])

        @pl.when(t + 1 < heads)
        def _():
            for f in fetches(t + 1):
                f.wait()
            project(t + 1)
            kv_send(t + 1)

        both(g0, t + 5)

        @pl.when(t >= SP)
        def _():
            c = t - SP
            wo_chunk(c).wait()

            @pl.when(c > 0)
            def _():
                acc_out(c - 1).wait()

            def tile(i, _):
                rows = pl.ds(_al(i * B, 128), B)
                acc_s[rows, :] = _dot(o_s[0, rows, :], wo_c[...], 1, 0)

            lax.fori_loop(0, tokens // B, tile, None)
            acc_out(c).start()


        def other(i, _):
            src = jnp.where(i == 1, s - 1, i - 2)

            @pl.when(s >= i)
            def _():
                @pl.when((i > 1) | (s == 3))
                def _():
                    kv(t, src, 0, 5, to_left).wait_recv()

                @pl.when((i != 2) | (s != 3))
                def _():
                    kv(t, src, 1, 5, to_left).wait_recv()

                block(t, src, 0, strips)
                block(t, src, 1, strips)

            for n, stage, ahead in ((1, g3, 2), (2, g2, 3), (3, g1, 4)):
                @pl.when(i == n)
                def _():
                    both(stage, t + ahead)

        lax.fori_loop(1, SP, other, None)
        finish(t)
        kv_sent(t)
        both(sent, t)

        @pl.when(t >= SP)
        def _():
            o_out(t).start()

    lax.fori_loop(0, heads, step, None)

    for g in range(heads + LAG - 2, heads + LAG):
        if g > heads + 1:
            g3(1, g - LAG)
        g4(1, g - LAG)
    acc_out(SP - 1).wait()
    for g in range(heads - SP, heads):
        o_out(jnp.int32(g)).wait()
    for g in range(heads, heads + LAG):
        sent(1, g - LAG)


def _project_out(x_ref, acc_ref, o_ref, w_ref, y_ref):
    tokens = x_ref.shape[0]
    for m in range(0, tokens, tokens // 2):
        rows = slice(m, m + tokens // 2)
        y_ref[rows, :] = (x_ref[rows, :].astype(jnp.float32) + acc_ref[rows, :] + _dot(o_ref[rows, :], w_ref[0], 1, 0)).astype(jnp.bfloat16)


def solution(mesh):
    def step(x, gain, wq, wk, wv, wo):
        tokens, depth = x.shape
        heads, group = wk.shape[1] // HEAD, wq.shape[1] // wk.shape[1]
        freq = np.float32(THETA) ** (-np.arange(HEAD // 2, dtype=np.float32) / np.float32(HEAD // 2))
        freq = np.concatenate([freq, freq])[None, :]
        width, B = (group + 2) * HEAD, tokens // 2
        low, wide = jnp.bfloat16, jnp.float32
        half_o = wo.shape[0] // 2 * SP
        anywhere, vmem = pl.BlockSpec(memory_space=pl.ANY), pl.BlockSpec(memory_space=pltpu.VMEM)
        dma = pltpu.SemaphoreType.DMA
        flops = 2 * tokens * depth * (wq.shape[1] * 2 + 2 * wk.shape[1]) + 4 * tokens * tokens * wq.shape[1] * SP
        seen, acc, _, wo, _ = pl.pallas_call(
            functools.partial(_kernel, group),
            out_shape=[jax.ShapeDtypeStruct((tokens, half_o), low), jax.ShapeDtypeStruct(x.shape, wide), jax.ShapeDtypeStruct((heads, depth, width), low),
                       jax.ShapeDtypeStruct((2, half_o, depth), low), jax.ShapeDtypeStruct((heads, 2, B, width), wide)],
            in_specs=[anywhere, vmem, vmem, anywhere, anywhere, anywhere, anywhere],
            out_specs=[anywhere] * 5,
            scratch_shapes=[
                pltpu.VMEM((tokens, depth), low),
                pltpu.VMEM((2, tokens, half_o), low),
                pltpu.VMEM((SLOTS, SP, tokens, HEAD), low),
                pltpu.VMEM((SLOTS, SP, HEAD, tokens), low),
                pltpu.VMEM((2, group * tokens, HEAD), low),
                pltpu.VMEM((depth - depth // SP, width), low),
                pltpu.VMEM((2, B, width), wide),
                pltpu.VMEM((2, wo.shape[0] // 2, depth), low),
                pltpu.VMEM((half_o, depth // SP), low),
                pltpu.VMEM((tokens, depth // SP), wide),
                pltpu.VMEM((1, group * tokens), wide),
                pltpu.VMEM((HEAD + 8, group * tokens), wide),
                pltpu.VMEM((tokens, HEAD), wide),
                pltpu.VMEM((tokens, HEAD), wide),
                dma((2, heads)), dma((2, heads, 2)), dma((2, heads)), dma((2, heads)), dma((2, heads)),
                dma((heads, 6)), dma((heads, SP, 2)), dma((SP,)), dma((5,)), dma((2, 3)), dma((2,)), dma((SP,)), dma((2,)),
            ],
            compiler_params=pltpu.CompilerParams(collective_id=0, has_side_effects=True, vmem_limit_bytes=67043328),
            cost_estimate=pl.CostEstimate(flops=flops, transcendentals=tokens * tokens * 2 * heads * group, bytes_accessed=200 * 2**20),
        )(x, gain, freq, wq, wk, wv, wo)
        n = depth // 4
        return pl.pallas_call(
            _project_out,
            out_shape=jax.ShapeDtypeStruct(x.shape, low),
            grid=(depth // n,),
            in_specs=[pl.BlockSpec((tokens, n), lambda i: (0, i)), pl.BlockSpec((tokens, n), lambda i: (0, i)),
                      pl.BlockSpec((tokens, half_o), lambda i: (0, 0)), pl.BlockSpec((1, half_o, n), lambda i: (1, 0, i))],
            out_specs=pl.BlockSpec((tokens, n), lambda i: (0, i)),
            compiler_params=pltpu.CompilerParams(dimension_semantics=("arbitrary",), vmem_limit_bytes=60 * 2**20),
            cost_estimate=pl.CostEstimate(flops=2 * tokens * half_o * depth, transcendentals=0, bytes_accessed=40 * 2**20),
        )(x, acc, seen, wo)

    tokens, whole = P(("dp", "sp"), None), P("sp", None)
    return jax.shard_map(
        step,
        mesh=mesh,
        in_specs=(tokens, P(None), whole, whole, whole, whole),
        out_specs=tokens,
        check_vma=False,
    )
```
